256 devices in a mesh: row: 64 (over z, y, core), kk: 4 (over x).
Axes of the slice: x: 4, y: 4, z: 8, core: 2. Of those that a mesh axis runs over, the one named last changes fastest.
Arguments:
- left_blocks: bfloat16 [32768, 4096], P('row', 'kk'), may hold values from -6 to 6
- right_blocks: bfloat16 [4096, 8192], P('kk', 'row'), may hold values from -0.125 to 0.125
- left_mask: int32 [256, 32], P('row', 'kk'), may hold values 0 or 1
- right_mask: int32 [32, 64], P('kk', 'row'), may hold values 0 or 1
- out_mask: int32 [256, 64], P('row'), may hold values 0 or 1
Outputs:
- product_blocks: bfloat16 [32768, 8192], P(('row', 'kk'))
The draws below stay inside these ranges and needn't reach their ends.
All inputs are finite; a program needn't handle non-finite values. No bound on the sum of `left_mask` or of `right_mask` or of `out_mask` on one device may be relied on, other than what follows from the above.
Results may differ from the reference program's by a relative error of at most 0.001.
Values may be sent and summed in bfloat16 or wider, within the bound.
No kernel may reach another device: no remote copies, remote signals or barrier semaphores. Data moves between devices by JAX's collectives and lax.ppermute only.
A program may use at most 192 MiB of HBM per device.

```python
import jax
import jax.numpy as jnp

BS = 128
KB = 32
IB = 256
JB = 64


def with_ends(values, key, least, top_value):
    shape = values.shape
    spot = [jax.random.randint(jax.random.fold_in(key, axis), (), 0, shape[axis]) for axis in range(len(shape))]
    values = values.at[tuple(spot)].set(least)
    longest = shape.index(max(shape))
    spot[longest] = (spot[longest] + 1) % shape[longest]
    return values.at[tuple(spot)].set(top_value)


def steps_of(rng, extent, split, least, high):
    gain = 1.0
    for axis_at, shards_of in split:
        draws = jax.random.uniform(jax.random.fold_in(jax.random.fold_in(rng, 6), axis_at), (shards_of,), jnp.float32, least / len(split), high / len(split))
        gain = gain * jnp.repeat(jnp.exp(draws), extent[axis_at] // shards_of).reshape((-1,) + (1,) * (len(extent) - 1 - axis_at))
    return gain


def normal_values(stream_key, dims, deviation, most, split=(), kind=jnp.bfloat16):
    entries = jax.random.normal(stream_key, dims, jnp.float32) * deviation
    if len(split) > 0:
        entries = steps_of(stream_key, dims, split, -0.22, 0.18) * entries
    return jnp.clip(entries, min=-most, max=most).astype(kind)


def setup_inputs(seed: int = 0) -> dict:
    key_list = jax.random.split(jax.random.key(seed), 6)
    return {
        "left_blocks": normal_values(key_list[0], (IB * BS, KB * BS), 1.0, 6.0, ((0, 64), (1, 4))),
        "right_blocks": normal_values(key_list[1], (KB * BS, JB * BS), (KB * BS // 2) ** -0.5, 0.125, ((0, 4), (1, 64))),
        "left_mask": with_ends((jax.random.randint(key_list[2], (IB, KB), 0, 2) < 1).astype(jnp.int32), jax.random.fold_in(key_list[2], 1), 0, 1),
        "right_mask": with_ends((jax.random.randint(key_list[3], (KB, JB), 0, 2) < 1).astype(jnp.int32), jax.random.fold_in(key_list[3], 1), 0, 1),
        "out_mask": with_ends((jax.random.randint(key_list[4], (IB, JB), 0, 4) < 3).astype(jnp.int32), jax.random.fold_in(key_list[4], 1), 0, 1),
    }


def expand(mask, size):
    return jnp.repeat(jnp.repeat(mask, size, axis=0), size, axis=1)


def reference(left_blocks, right_blocks, left_mask, right_mask, out_mask):
    left_used = left_blocks * expand(left_mask, BS).astype(jnp.bfloat16)
    right_used = right_blocks * expand(right_mask, BS).astype(jnp.bfloat16)
    full = jnp.dot(left_used, right_used, preferred_element_type=jnp.float32)
    return (full * expand(out_mask, BS).astype(jnp.float32)).astype(jnp.bfloat16)
```

```python
import functools

import jax
import jax.numpy as jnp
from jax import lax
from jax.experimental import pallas as pl
from jax.experimental.pallas import tpu as pltpu
from jax.sharding import PartitionSpec as P

Z, Y, C, X = 8, 4, 2, 4
BS = 128
BOTH = ("row", "kk")


def flat(z, y, c, x):
    return ((z * Y + y) * C + c) * X + x


def move(v, source):
    pairs = []
    for z in range(Z):
        for y in range(Y):
            for c in range(C):
                for x in range(X):
                    sz, sy, sc, sx = source(z, y, c, x)
                    pairs.append((flat(sz % Z, sy % Y, sc, sx), flat(z, y, c, x)))
    return lax.ppermute(v, BOTH, pairs)


def from_y(v, d):
    return move(v, lambda z, y, c, x: (z, y + d, c, x))


def from_z(v, d):
    return move(v, lambda z, y, c, x: (z + d, y, c, x))


def from_share(v):
    return move(v, lambda z, y, c, x: (z, y, c, x ^ 1))


def from_reduce(v):
    return move(v, lambda z, y, c, x: (z, y, c, X - 1 - x))


def from_core(v):
    return move(v, lambda z, y, c, x: (z, y, 1 - c, x))


def mask_right(right, mask):
    depth, cols = right.shape
    blocks = mask.shape[0]

    def body(mask_ref, right_ref, out_ref):
        for k in range(blocks):
            rows = pl.ds(k * BS, BS)
            out_ref[rows, :] = right_ref[rows, :] * mask_ref[k, 0].astype(jnp.float32).astype(jnp.bfloat16)

    return pl.pallas_call(
        body,
        out_shape=jax.ShapeDtypeStruct((depth, cols), jnp.bfloat16),
        in_specs=[pl.BlockSpec(memory_space=pltpu.SMEM), pl.BlockSpec(memory_space=pltpu.VMEM)],
        out_specs=pl.BlockSpec(memory_space=pltpu.VMEM),
        name="mask_right",
    )(mask, right)


def mask_left(left, mask, order):
    depth = left.shape[1]

    def body(order_ref, mask_ref, a_ref, b_ref, mine_ref, theirs_ref):
        i = pl.program_id(0)
        for src, dst, at in ((a_ref, mine_ref, order_ref[i]), (b_ref, theirs_ref, order_ref[i + 2])):
            for k in range(depth // BS):
                cols = pl.ds(k * BS, BS)
                dst[:, cols] = src[:, cols] * mask_ref[at, k].astype(jnp.float32).astype(jnp.bfloat16)

    out = jax.ShapeDtypeStruct((2 * BS, depth), jnp.bfloat16)
    return pl.pallas_call(
        body,
        out_shape=(out, out),
        grid_spec=pltpu.PrefetchScalarGridSpec(
            num_scalar_prefetch=2,
            grid=(2,),
            in_specs=[
                pl.BlockSpec((BS, depth), lambda i, o, m: (o[i], 0)),
                pl.BlockSpec((BS, depth), lambda i, o, m: (o[i + 2], 0)),
            ],
            out_specs=[pl.BlockSpec((BS, depth), lambda i, o, m: (i, 0))] * 2,
        ),
        name="mask_left",
    )(order, mask, left, left)


def partial_product(lhs, own, others):
    rows, depth2 = lhs.shape
    depth, quarter = depth2 // 2, rows // 4
    planes = len(own)
    halves = [(p, h, a) for p, parts in enumerate(own) for h, a in enumerate(parts)]

    def body(lhs_ref, *refs):
        own_refs, line_refs, (send_ref, keep_ref) = refs[: len(halves)], refs[len(halves) : -2], refs[-2:]

        def step(o, a, b):
            w1 = jnp.concatenate([o[0], o[1]], axis=1)
            w2 = jnp.concatenate([a[0], b[0]], axis=1)
            out = jnp.dot(lhs_ref[:, :depth], w1, preferred_element_type=jnp.float32)
            out += jnp.dot(lhs_ref[:, depth:], w2, preferred_element_type=jnp.float32)
            send_ref[:quarter, :] = out[:quarter]
            keep_ref[:quarter, :] = out[quarter : 2 * quarter]
            send_ref[quarter:, :] = out[2 * quarter : 3 * quarter]
            keep_ref[quarter:, :] = out[3 * quarter :]

        i = pl.program_id(0)
        for (p, h, a), ref in zip(halves, own_refs):
            for k in range(a.shape[0] // 2):
                at = h + k
                pl.when(i == 2 * p + at)(functools.partial(step, ref, line_refs[2 * at], line_refs[2 * at + 1]))

    def own_spec(p, h, a):
        if a.shape[0] == 2:
            return pl.BlockSpec((2, depth, BS), lambda i: (0, 0, 0))
        return pl.BlockSpec((2, depth, BS), lambda i: (jnp.clip(i - 2 * p, 0, 1), 0, 0))

    out = jax.ShapeDtypeStruct((2 * quarter, planes * Y * BS), jnp.float32)
    half = pl.BlockSpec((2 * quarter, 2 * BS), lambda i: (0, i))
    return pl.pallas_call(
        body,
        grid=(2 * planes,),
        out_shape=(out, out),
        in_specs=[pl.BlockSpec((rows, depth2), lambda i: (0, 0))]
        + [own_spec(*t) for t in halves]
        + [pl.BlockSpec((1, depth, BS), lambda i: (i // 2, 0, 0))] * Y,
        out_specs=(half, half),
        cost_estimate=pl.CostEstimate(
            flops=2 * rows * depth2 * planes * Y * BS, bytes_accessed=(2 + 3 * planes) << 20, transcendentals=0
        ),
        name="partial_product",
    )(lhs, *(a for _, _, a in halves), *others)


def finish(keep, got):
    half, cols = keep.shape[0] // 2, keep.shape[1]
    width = 2 * BS

    def body(keep_ref, got_ref, own_ref, other_ref):
        total = (keep_ref[...] + got_ref[...]).astype(jnp.bfloat16)
        own_ref[...] = total[:half]
        other_ref[...] = total[half:]

    out = jax.ShapeDtypeStruct((half, cols), jnp.bfloat16)
    return pl.pallas_call(
        body,
        grid=(cols // width,),
        out_shape=(out, out),
        in_specs=[pl.BlockSpec((2 * half, width), lambda i: (0, i))] * 2,
        out_specs=[pl.BlockSpec((half, width), lambda i: (0, i))] * 2,
        cost_estimate=pl.CostEstimate(flops=keep.size * 2, bytes_accessed=keep.size * 10, transcendentals=0),
        name="finish",
    )(keep, got)


def assemble(where, out_mask, own, other, slots):
    rows = own[0].shape[0]
    count = len(slots)

    def body(where_ref, mask_ref, *refs):
        out_ref = refs[-1]
        z, y, c, x = (where_ref[i] for i in range(4))
        for s, planes in enumerate(slots):
            for p, d in enumerate(planes):
                for k in range(Y):
                    group = lax.rem(z + d % Z, Z) * Y + lax.rem(y + k, Y)
                    for src, core in ((refs[s], c), (refs[count + s], 1 - c)):
                        block = group * C + core
                        cols = pl.ds(pl.multiple_of(block * BS, BS), BS)
                        scale = mask_ref[x, block].astype(jnp.float32).astype(jnp.bfloat16)
                        out_ref[:, cols] = src[:, pl.ds((p * Y + k) * BS, BS)] * scale

    smem = pl.BlockSpec(memory_space=pltpu.SMEM)
    vmem = pl.BlockSpec(memory_space=pltpu.VMEM)
    return pl.pallas_call(
        body,
        out_shape=jax.ShapeDtypeStruct((rows, Z * Y * C * BS), jnp.bfloat16),
        in_specs=[smem, smem] + [vmem] * (2 * count),
        out_specs=vmem,
        name="assemble",
    )(where, out_mask, *own, *other)


def after(value, *earlier):
    return lax.optimization_barrier((value, *earlier))[0]


def per_device(left_blocks, right_blocks, left_mask, right_mask, out_mask):
    row, x = lax.axis_index("row"), lax.axis_index("kk")
    z, y, c = row // (Y * C), (row // C) % Y, row % C
    where = jnp.stack([z, y, c, x]).astype(jnp.int32)
    near = x + 1 - 2 * (x % 2)
    order = jnp.stack([X - 1 - x, x, X - 1 - near, near]).astype(jnp.int32)

    mine = mask_right(right_blocks, right_mask)
    theirs = from_share(mine)
    along = [from_y(mine, d) for d in range(1, Y)]

    own_rows, their_rows = mask_left(left_blocks, left_mask, order)
    got_rows = from_share(after(their_rows, mine))

    def spread(v):
        return [from_y(v, d) for d in range(1, Y)]

    line = {1: from_z(theirs, 1), -1: from_z(theirs, -1)}
    others = [[theirs[None]] + spread(theirs[None])]

    own0 = jnp.stack([mine] + [after(v, theirs) for v in along])
    own = {0: own0, 1: from_z(own0, 1), -1: from_z(own0, -1)}

    def pair(d):
        return jnp.stack([line[d], line[-d]])

    b1 = after(pair(1), own0)
    line[2], line[-2] = from_z(after(line[1], own0), 1), from_z(after(line[-1], own0), -1)
    others.append([b1] + spread(b1))

    half = jnp.concatenate([own_rows, after(got_rows, b1)], axis=1)
    lhs = jnp.concatenate([half, from_core(half)], axis=0)

    b2 = after(pair(2), lhs)
    line[3], line[-3] = from_z(after(line[2], lhs), 1), from_z(after(line[-2], lhs), -1)

    sends, keeps, gots = [], [], []

    def multiply(slot, parts):
        send, keep = partial_product(lhs, parts, others[slot])
        sends.append(send)
        keeps.append(keep)
        gots.append(from_reduce(send))

    others[0] = [after(v, b2) for v in others[0]]
    multiply(0, [[own0]])

    others.append([b2] + spread(b2))
    own[2], own[-2] = from_z(after(own[1], sends[0]), 1), from_z(after(own[-1], sends[0]), -1)
    b3 = after(pair(3), sends[0])
    line[4] = from_z(after(line[3], sends[0]), 1)

    others[1] = [after(v, b3) for v in others[1]]
    multiply(1, [[own[1]], [own[-1]]])
    b3 = after(b3, sends[1])
    others.append([b3] + spread(b3))
    own[3], own[-3] = from_z(after(own[2], sends[1]), 1), from_z(after(own[-2], sends[1]), -1)
    last = after(line[4], sends[1])[None]
    others.append([last] + spread(last))

    ends = [finish(keeps[0], after(gots[0], sends[1]))]
    others[2] = [after(v, ends[0][0]) for v in others[2]]
    multiply(2, [[own[2]], [own[-2]]])
    own4 = [
        from_z(after(own[3], sends[2])[: Y // 2], 1),
        from_z(after(own[-3], sends[2])[Y // 2 :], -1),
    ]
    ends.append(finish(keeps[1], after(gots[1], sends[2])))
    others[3] = [after(v, ends[1][0], *own4) for v in others[3]]
    multiply(3, [[own[3]], [own[-3]]])
    others[4] = [after(v, sends[3]) for v in others[4]]
    multiply(4, [own4])
    ends.append(finish(keeps[2], after(gots[2], sends[4])))
    ends.append(finish(keeps[3], after(gots[3], ends[2][0])))
    ends.append(finish(keeps[4], after(gots[4], ends[3][0])))
    slots = [(0,), (1, -1), (2, -2), (3, -3), (4,)]
    return assemble(where, out_mask, [a for a, _ in ends], [from_core(b) for _, b in ends], slots)


def solution(mesh):
    in_specs = (P("row", "kk"), P("kk", "row"), P("row", "kk"), P("kk", "row"), P("row", None))
    out_specs = P(("row", "kk"), None)
    return jax.shard_map(
        per_device, mesh=mesh, in_specs=in_specs, out_specs=out_specs, check_vma=False
    )
```

```python
import functools

import jax
import jax.numpy as jnp
from jax import lax
from jax.experimental import pallas as pl
from jax.experimental.pallas import tpu as pltpu
from jax.sharding import PartitionSpec as P


Z, Y, C, X = 8, 4, 2, 4
BS = 128
BOTH = ("row", "kk")


def flat(z, y, c, x):
    return ((z * Y + y) * C + c) * X + x


def move(v, source):
    pairs = []
    for z in range(Z):
        for y in range(Y):
            for c in range(C):
                for x in range(X):
                    sz, sy, sc, sx = source(z, y, c, x)
                    pairs.append((flat(sz % Z, sy % Y, sc, sx), flat(z, y, c, x)))
    return lax.ppermute(v, BOTH, pairs)


def from_y(v, d):
    return move(v, lambda z, y, c, x: (z, y + d, c, x))


def from_z(v, d):
    return move(v, lambda z, y, c, x: (z + d, y, c, x))


def from_share(v):
    return move(v, lambda z, y, c, x: (z, y, c, x ^ 1))


def from_reduce(v):
    return move(v, lambda z, y, c, x: (z, y, c, X - 1 - x))


def from_core(v):
    return move(v, lambda z, y, c, x: (z, y, 1 - c, x))


def spread(v):
    return [from_y(v, d) for d in range(1, Y)]


def mask_right(right, mask):
    depth, cols = right.shape
    blocks = mask.shape[1]

    def body(mask_ref, right_ref, out_ref):
        for k in range(blocks):
            rows = pl.ds(k * BS, BS)
            out_ref[rows, :] = right_ref[rows, :] * mask_ref[0, k].astype(jnp.float32).astype(jnp.bfloat16)

    return pl.pallas_call(
        body,
        out_shape=jax.ShapeDtypeStruct((depth, cols), jnp.bfloat16),
        in_specs=[pl.BlockSpec(memory_space=pltpu.SMEM), pl.BlockSpec(memory_space=pltpu.VMEM)],
        out_specs=pl.BlockSpec(memory_space=pltpu.VMEM),
        name="mask_right",
    )(mask, right)


def mask_left(left, mask, order):
    depth = left.shape[1]

    def body(order_ref, mask_ref, a_ref, b_ref, mine_ref, theirs_ref):
        i = pl.program_id(0)
        for src, dst, at in ((a_ref, mine_ref, order_ref[i]), (b_ref, theirs_ref, order_ref[i + 2])):
            for k in range(depth // BS):
                cols = pl.ds(k * BS, BS)
                dst[:, cols] = src[:, cols] * mask_ref[at, k].astype(jnp.float32).astype(jnp.bfloat16)

    out = jax.ShapeDtypeStruct((2 * BS, depth), jnp.bfloat16)
    return pl.pallas_call(
        body,
        out_shape=(out, out),
        grid_spec=pltpu.PrefetchScalarGridSpec(
            num_scalar_prefetch=2,
            grid=(2,),
            in_specs=[
                pl.BlockSpec((BS, depth), lambda i, o, m: (o[i], 0)),
                pl.BlockSpec((BS, depth), lambda i, o, m: (o[i + 2], 0)),
            ],
            out_specs=[pl.BlockSpec((BS, depth), lambda i, o, m: (i, 0))] * 2,
        ),
        name="mask_left",
    )(order, mask, left, left)


def partial_product(lhs, own, others):
    rows, depth2 = lhs.shape
    depth, quarter = depth2 // 2, rows // 4
    planes, chunk = len(own), 512
    halves = [(p, h, a) for p, parts in enumerate(own) for h, a in enumerate(parts)]

    def body(lhs_ref, *refs):
        own_refs, line_refs, (send_ref, keep_ref, right_ref, total_ref) = refs[: len(halves)], refs[len(halves) : -4], refs[-4:]

        def fill(own_ref, a_ref, b_ref):
            right_ref[:depth, :BS] = own_ref[0]
            right_ref[:depth, BS:] = own_ref[1]
            right_ref[depth:, :BS] = a_ref[0]
            right_ref[depth:, BS:] = b_ref[0]

        i = pl.program_id(0)
        for (p, h, a), ref in zip(halves, own_refs):
            for k in range(a.shape[0] // 2):
                at = h + k
                pl.when(i == 2 * p + at)(functools.partial(fill, ref, line_refs[2 * at], line_refs[2 * at + 1]))
        total_ref[...] = jnp.dot(lhs_ref[:, :chunk], right_ref[:chunk, :], preferred_element_type=jnp.float32)

        def add(k, _):
            at = pl.ds(pl.multiple_of(k * chunk, chunk), chunk)
            total_ref[...] += jnp.dot(lhs_ref[:, at], right_ref[at, :], preferred_element_type=jnp.float32)
            return 0

        lax.fori_loop(1, depth2 // chunk, add, 0)
        out = total_ref[...]
        send_ref[:quarter, :] = out[:quarter]
        keep_ref[:quarter, :] = out[quarter : 2 * quarter]
        send_ref[quarter:, :] = out[2 * quarter : 3 * quarter]
        keep_ref[quarter:, :] = out[3 * quarter :]

    def own_spec(p, h, a):
        if a.shape[0] == 2:
            return pl.BlockSpec((2, depth, BS), lambda i: (0, 0, 0))
        return pl.BlockSpec((2, depth, BS), lambda i: (jnp.clip(i - 2 * p, 0, 1), 0, 0))

    out = jax.ShapeDtypeStruct((2 * quarter, planes * Y * BS), jnp.float32)
    half = pl.BlockSpec((2 * quarter, 2 * BS), lambda i: (0, i))
    return pl.pallas_call(
        body,
        grid=(2 * planes,),
        out_shape=(out, out),
        in_specs=[pl.BlockSpec((rows, depth2), lambda i: (0, 0))]
        + [own_spec(*t) for t in halves]
        + [pl.BlockSpec((1, depth, BS), lambda i: (i // 2, 0, 0))] * Y,
        out_specs=(half, half),
        scratch_shapes=[pltpu.VMEM((depth2, 2 * BS), jnp.bfloat16), pltpu.VMEM((rows, 2 * BS), jnp.float32)],
        cost_estimate=pl.CostEstimate(
            flops=2 * rows * depth2 * planes * Y * BS, bytes_accessed=(2 + 3 * planes) << 20, transcendentals=0
        ),
        name="partial_product",
    )(lhs, *(a for _, _, a in halves), *others)


def finish(keep, got):
    half, cols = keep.shape[0] // 2, keep.shape[1]
    width = 2 * BS

    def body(keep_ref, got_ref, own_ref, other_ref):
        total = (keep_ref[...] + got_ref[...]).astype(jnp.bfloat16)
        own_ref[...] = total[:half]
        other_ref[...] = total[half:]

    out = jax.ShapeDtypeStruct((half, cols), jnp.bfloat16)
    return pl.pallas_call(
        body,
        grid=(cols // width,),
        out_shape=(out, out),
        in_specs=[pl.BlockSpec((2 * half, width), lambda i: (0, i))] * 2,
        out_specs=[pl.BlockSpec((half, width), lambda i: (0, i))] * 2,
        cost_estimate=pl.CostEstimate(flops=keep.size * 2, bytes_accessed=keep.size * 10, transcendentals=0),
        name="finish",
    )(keep, got)


def assemble(out_mask, own, other, slots):
    rows = own[0].shape[0]
    count = len(slots)

    def body(mask_ref, *refs):
        out_ref = refs[-1]
        z, y, c, x = position()
        for s, planes in enumerate(slots):
            for p, d in enumerate(planes):
                for k in range(Y):
                    group = lax.rem(z + d % Z, Z) * Y + lax.rem(y + k, Y)
                    for src, core in ((refs[s], c), (refs[count + s], 1 - c)):
                        block = group * C + core
                        cols = pl.ds(pl.multiple_of(block * BS, BS), BS)
                        scale = mask_ref[x, block].astype(jnp.float32).astype(jnp.bfloat16)
                        out_ref[:, cols] = src[:, pl.ds((p * Y + k) * BS, BS)] * scale

    smem = pl.BlockSpec(memory_space=pltpu.SMEM)
    vmem = pl.BlockSpec(memory_space=pltpu.VMEM)
    return pl.pallas_call(
        body,
        out_shape=jax.ShapeDtypeStruct((rows, Z * Y * C * BS), jnp.bfloat16),
        in_specs=[smem] + [vmem] * (2 * count),
        out_specs=vmem,
        name="assemble",
    )(out_mask, *own, *other)


def position():
    row, x = lax.axis_index("row"), lax.axis_index("kk")
    return row // (Y * C), (row // C) % Y, row % C, x


SLOTS = [(0,), (1, -1), (2, -2), (3, -3), (4,)]


def per_device(left_blocks, right_blocks, left_mask, right_mask, out_mask):
    x = lax.axis_index("kk")
    near = x + 1 - 2 * (x % 2)
    order = jnp.stack([X - 1 - x, x, X - 1 - near, near]).astype(jnp.int32)

    mine = mask_right(right_blocks, right_mask.T)
    line = {0: from_share(mine)}
    own = {0: jnp.stack([mine] + spread(mine))}
    for d in (1, 2, 3):
        for s in (1, -1):
            line[s * d] = from_z(line[s * (d - 1)], s)
            own[s * d] = from_z(own[s * (d - 1)], s)
    line[4] = from_z(line[3], 1)
    own4 = [from_z(own[3][: Y // 2], 1), from_z(own[-3][Y // 2 :], -1)]

    own_rows, their_rows = mask_left(left_blocks, left_mask, order)
    half = jnp.concatenate([own_rows, from_share(their_rows)], axis=1)
    lhs = jnp.concatenate([half, from_core(half)], axis=0)

    own_ends, other_ends = [], []
    for planes in SLOTS:
        first = jnp.stack([line[d] for d in planes])
        others = [first] + spread(first)
        parts = [own4] if planes == (4,) else [[own[d]] for d in planes]
        send, keep = partial_product(lhs, parts, others)
        got = from_reduce(send)
        a, b = finish(keep, got)
        own_ends.append(a)
        other_ends.append(from_core(b))
    return assemble(out_mask, own_ends, other_ends, SLOTS)


def solution(mesh):
    in_specs = (P("row", "kk"), P("kk", "row"), P("row", "kk"), P("kk", "row"), P("row", None))
    out_specs = P(("row", "kk"), None)

    return jax.shard_map(per_device, mesh=mesh, in_specs=in_specs, out_specs=out_specs, check_vma=False)
```

```python
import jax
import jax.numpy as jnp
from jax import lax
from jax.experimental import pallas as pl
from jax.experimental.pallas import tpu as pltpu
from jax.sharding import PartitionSpec as P


Z, Y, C, X = 8, 4, 2, 4
BS = 128
BOTH = ("row", "kk")


def flat(z, y, c, x):
    return ((z * Y + y) * C + c) * X + x


def move(v, source):
    pairs = []
    for z in range(Z):
        for y in range(Y):
            for c in range(C):
                for x in range(X):
                    sz, sy, sc, sx = source(z, y, c, x)
                    pairs.append((flat(sz % Z, sy % Y, sc, sx), flat(z, y, c, x)))
    return lax.ppermute(v, BOTH, pairs)


def from_y(v, d):
    return move(v, lambda z, y, c, x: (z, y + d, c, x))


def from_z(v, d):
    return move(v, lambda z, y, c, x: (z + d, y, c, x))


def from_share(v):
    return move(v, lambda z, y, c, x: (z, y, c, x ^ 1))


def from_reduce(v):
    return move(v, lambda z, y, c, x: (z, y, c, X - 1 - x))


def from_core(v):
    return move(v, lambda z, y, c, x: (z, y, 1 - c, x))


def spread(v):
    return [from_y(v, d) for d in range(1, Y)]


def mask_right(right, mask):
    depth, cols = right.shape
    blocks = mask.shape[1]

    def body(mask_ref, right_ref, out_ref):
        for k in range(blocks):
            rows = pl.ds(k * BS, BS)
            out_ref[rows, :] = right_ref[rows, :] * mask_ref[0, k].astype(jnp.float32).astype(jnp.bfloat16)

    return pl.pallas_call(
        body,
        out_shape=jax.ShapeDtypeStruct((depth, cols), jnp.bfloat16),
        in_specs=[pl.BlockSpec(memory_space=pltpu.SMEM), pl.BlockSpec(memory_space=pltpu.VMEM)],
        out_specs=pl.BlockSpec(memory_space=pltpu.VMEM),
        name="mask_right",
    )(mask, right)


def mask_left(left, mask, order):
    depth = left.shape[1]

    def body(order_ref, mask_ref, a_ref, b_ref, mine_ref, theirs_ref):
        i = pl.program_id(0)
        for src, dst, at in ((a_ref, mine_ref, order_ref[i]), (b_ref, theirs_ref, order_ref[i + 2])):
            for k in range(depth // BS):
                cols = pl.ds(k * BS, BS)
                dst[:, cols] = src[:, cols] * mask_ref[at, k].astype(jnp.float32).astype(jnp.bfloat16)

    out = jax.ShapeDtypeStruct((2 * BS, depth), jnp.bfloat16)
    return pl.pallas_call(
        body,
        out_shape=(out, out),
        grid_spec=pltpu.PrefetchScalarGridSpec(
            num_scalar_prefetch=2,
            grid=(2,),
            in_specs=[
                pl.BlockSpec((BS, depth), lambda i, o, m: (o[i], 0)),
                pl.BlockSpec((BS, depth), lambda i, o, m: (o[i + 2], 0)),
            ],
            out_specs=[pl.BlockSpec((BS, depth), lambda i, o, m: (i, 0))] * 2,
        ),
        name="mask_left",
    )(order, mask, left, left)


TAIL = 16


def code(v):
    return jnp.clip(jnp.floor(v + 0.5), -32767.0, 32767.0).astype(jnp.int32).astype(jnp.int16)


def value(q):
    return q.astype(jnp.int32).astype(jnp.float32)


def partial_product(lhs, steps):
    rows, depth2 = lhs.shape
    depth, quarter, width, count = depth2 // 2, rows // 4, 2 * BS, len(steps)
    arrays = []
    for step in steps:
        for a, _ in step:
            if not any(a is b for b in arrays):
                arrays.append(a)

    def which(a):
        return next(i for i, b in enumerate(arrays) if a is b)

    def body(lhs_ref, *refs):
        ins, (send_ref, keep_ref, right_ref, send_buf, keep_buf, in_sem, out_sem) = refs[: len(arrays)], refs[len(arrays) :]

        def load(src, i, j):
            dst = right_ref.at[i, pl.ds((j // 2) * depth, depth), pl.ds((j % 2) * BS, BS)]
            return pltpu.make_async_copy(src, dst, in_sem.at[i, j])

        for i, step in enumerate(steps):
            for j, (a, k) in enumerate(step):
                ref = ins[which(a)]
                load(ref if k is None else ref.at[k], i, j).start()

        def store(i):
            cols = pl.ds(pl.multiple_of(i * width, width), width)
            return (
                pltpu.make_async_copy(send_buf.at[i], send_ref.at[:, cols], out_sem.at[i, 0]),
                pltpu.make_async_copy(keep_buf.at[i], keep_ref.at[:, cols], out_sem.at[i, 1]),
            )

        def multiply(i, _):
            first, at = steps[0][0]
            for j in range(4):
                ref = ins[which(first)]
                load(ref if at is None else ref.at[at], i, j).wait()
            out = jnp.dot(lhs_ref[...], right_ref[i], preferred_element_type=jnp.float32)
            keep_buf[i, :quarter, :] = out[quarter : 2 * quarter]
            keep_buf[i, quarter:, :] = out[3 * quarter :]
            upper, lower = out[:quarter], out[2 * quarter : 3 * quarter]
            most = jnp.max(jnp.maximum(jnp.abs(upper), jnp.abs(lower)), axis=0, keepdims=True)
            exponent = jnp.ceil(jnp.log2(jnp.maximum(most, 1e-30)))
            scale = jnp.exp2(15.0 - exponent)
            send_buf[i, :quarter, :] = code(upper * scale)
            send_buf[i, quarter : 2 * quarter, :] = code(lower * scale)
            send_buf[i, 2 * quarter :, :] = code(jnp.broadcast_to(exponent, (TAIL, width)))
            for copy in store(i):
                copy.start()
            return 0

        lax.fori_loop(0, count, multiply, 0)
        for i in range(count):
            for copy in store(i):
                copy.wait()

    sent = jax.ShapeDtypeStruct((2 * quarter + TAIL, count * width), jnp.int16)
    kept = jax.ShapeDtypeStruct((2 * quarter, count * width), jnp.float32)
    anywhere = pl.BlockSpec(memory_space=pltpu.HBM)
    return pl.pallas_call(
        body,
        out_shape=(sent, kept),
        in_specs=[pl.BlockSpec(memory_space=pltpu.VMEM)] + [anywhere] * len(arrays),
        out_specs=(anywhere, anywhere),
        scratch_shapes=[
            pltpu.VMEM((count, depth2, width), jnp.bfloat16),
            pltpu.VMEM((count, 2 * quarter + TAIL, width), jnp.int16),
            pltpu.VMEM((count, 2 * quarter, width), jnp.float32),
            pltpu.SemaphoreType.DMA((count, 4)),
            pltpu.SemaphoreType.DMA((count, 2)),
        ],
        cost_estimate=pl.CostEstimate(
            flops=2 * rows * depth2 * count * width, bytes_accessed=(3 * count) << 19, transcendentals=0
        ),
        name="partial_product",
    )(lhs, *arrays)


def finish(parts):
    rows = parts[0][0].shape[0]
    half, count = rows // 2, len(parts)
    widths = [k.shape[1] for k, _ in parts]
    starts = [sum(widths[:i]) for i in range(count)]
    total = sum(widths)
    tall = 32

    def body(*refs):
        ins, (own_ref, other_ref, a_buf, b_buf, own_buf, other_buf, in_sem, out_sem) = refs[: 2 * count], refs[2 * count :]
        loads, stores = [], []
        for i in range(count):
            cols = pl.ds(starts[i], widths[i])
            loads.append(
                (
                    pltpu.make_async_copy(ins[2 * i], a_buf.at[:, cols], in_sem.at[i, 0]),
                    pltpu.make_async_copy(ins[2 * i + 1], b_buf.at[:, cols], in_sem.at[i, 1]),
                )
            )
            stores.append(
                (
                    pltpu.make_async_copy(own_buf.at[:, cols], own_ref.at[:, cols], out_sem.at[i, 0]),
                    pltpu.make_async_copy(other_buf.at[:, cols], other_ref.at[:, cols], out_sem.at[i, 1]),
                )
            )
        for pair in loads:
            for copy in pair:
                copy.start()
        for i in range(count):
            for copy in loads[i]:
                copy.wait()
            cols = pl.ds(starts[i], widths[i])
            unit = jnp.exp2(value(b_buf[rows:, cols])[:1] - 15.0)
            for base, dst in ((0, own_buf), (half, other_buf)):

                def add(r, _, base=base, dst=dst, cols=cols, unit=unit):
                    src = pl.ds(pl.multiple_of(base + r * tall, tall), tall)
                    to = pl.ds(pl.multiple_of(r * tall, tall), tall)
                    dst[to, cols] = (a_buf[src, cols] + value(b_buf[src, cols]) * unit).astype(jnp.bfloat16)
                    return 0

                lax.fori_loop(0, half // tall, add, 0)
            for copy in stores[i]:
                copy.start()
        for pair in stores:
            for copy in pair:
                copy.wait()

    out = jax.ShapeDtypeStruct((half, total), jnp.bfloat16)
    anywhere = pl.BlockSpec(memory_space=pltpu.HBM)
    return pl.pallas_call(
        body,
        out_shape=(out, out),
        in_specs=[anywhere] * (2 * count),
        out_specs=(anywhere, anywhere),
        scratch_shapes=[pltpu.VMEM((rows, total), jnp.float32), pltpu.VMEM((rows + TAIL, total), jnp.int16)]
        + [pltpu.VMEM((half, total), jnp.bfloat16)] * 2
        + [pltpu.SemaphoreType.DMA((count, 2))] * 2,
        cost_estimate=pl.CostEstimate(flops=rows * total * 2, bytes_accessed=rows * total * 10, transcendentals=0),
        name="finish",
    )(*(v for pair in parts for v in pair))


def place(out_mask, base, own, other, groups):
    rows = own[0].shape[0]
    count = len(groups)
    blocks = 4 * sum(len(steps) for steps in groups)

    def body(mask_ref, *refs):
        ends, (out_ref, buf, sem) = refs[-3 - 2 * count : -3], refs[-3:]
        z, y, c, x = position()
        copies = []
        for g, steps in enumerate(groups):
            for p, (d, h) in enumerate(steps):
                for k in range(2):
                    group = lax.rem(z + d % Z, Z) * Y + lax.rem(y + 2 * h + k, Y)
                    for src, core in ((ends[g], c), (ends[count + g], 1 - c)):
                        i, block = len(copies), group * C + core
                        scale = mask_ref[x, block].astype(jnp.float32).astype(jnp.bfloat16)
                        buf[i] = src[:, pl.ds((2 * p + k) * BS, BS)] * scale
                        cols = pl.ds(pl.multiple_of(block * BS, BS), BS)
                        copies.append(pltpu.make_async_copy(buf.at[i], out_ref.at[:, cols], sem.at[i]))
                        copies[-1].start()
        for copy in copies:
            copy.wait()

    smem, vmem, hbm = (pl.BlockSpec(memory_space=m) for m in (pltpu.SMEM, pltpu.VMEM, pltpu.HBM))
    bases = [] if base is None else [base]
    return pl.pallas_call(
        body,
        out_shape=jax.ShapeDtypeStruct((rows, Z * Y * C * BS), jnp.bfloat16),
        in_specs=[smem] + [hbm] * len(bases) + [vmem] * (2 * count),
        out_specs=hbm,
        input_output_aliases={1: 0} if bases else {},
        scratch_shapes=[pltpu.VMEM((blocks, rows, BS), jnp.bfloat16), pltpu.SemaphoreType.DMA((blocks,))],
        cost_estimate=pl.CostEstimate(flops=blocks * rows * BS, bytes_accessed=blocks * rows * BS * 4, transcendentals=0),
        name="place",
    )(out_mask, *bases, *own, *other)


def position():
    row, x = lax.axis_index("row"), lax.axis_index("kk")
    return row // (Y * C), (row // C) % Y, row % C, x


PAIRS = range(Y // 2)
SLOTS = {
    "0": [(0, h) for h in PAIRS],
    "4": [(4, h) for h in PAIRS],
    "1": [(d, h) for d in (1, -1) for h in PAIRS],
    "2": [(d, h) for d in (2, -2) for h in PAIRS],
    "3": [(d, h) for d in (3, -3) for h in PAIRS],
}
GROUPS = {"fin0": ("0", "1"), "fin1": ("2", "4"), "fin2": ("3",)}


def per_device(left_blocks, right_blocks, left_mask, right_mask, out_mask):
    x = lax.axis_index("kk")
    near = x + 1 - 2 * (x % 2)
    order = jnp.stack([X - 1 - x, x, X - 1 - near, near]).astype(jnp.int32)

    mine = mask_right(right_blocks, right_mask.T)
    theirs = from_share(mine)
    along = spread(mine)
    far = from_z(mine, 4)
    near_along = from_share(jnp.stack(along))
    own = {}
    line = {(0, 0): (theirs, None)}
    for k in range(1, Y):
        line[0, k] = (near_along, k - 1)

    hop = {}
    for s in (1, -1):
        first = from_z(theirs, s)
        line[s, 0] = (first, None)
        hop[s, 0] = jnp.stack([mine, *along, first])
        for d in (1, 2):
            packet = from_z(hop[s, d - 1], s)
            hop[s, d] = packet
            for k in range(Y):
                own[s * d, k] = (packet, k)
            line[s * (d + 1), 0] = (packet, Y)
        last = hop[s, 2][:Y]
        packet = from_z(last, s)
        for k in range(Y):
            own[s * 3, k] = (packet, k)
    for k in range(Y):
        own[0, k] = (hop[1, 0], k)

    def block(pair):
        array, index = pair
        return array if index is None else array[index]

    for d in (1, 2, 3):
        both = jnp.stack([block(line[d, 0]), block(line[-d, 0])])
        for k, got in enumerate(spread(both), 1):
            line[d, k], line[-d, k] = (got, 0), (got, 1)

    far_all = [far] + spread(far)
    near_far = from_share(jnp.stack(far_all))
    for k in range(Y):
        own[4, k], line[4, k] = (far_all[k], None), (near_far, k)

    own_rows, their_rows = mask_left(left_blocks, left_mask, order)
    half = jnp.concatenate([own_rows, from_share(their_rows)], axis=1)
    lhs = jnp.concatenate([half, from_core(half)], axis=0)

    sums = {}
    for slot, steps in SLOTS.items():
        send, keep = partial_product(
            lhs, [[table[d, 2 * h + k] for table in (own, line) for k in range(2)] for d, h in steps]
        )
        sums[slot] = (keep, from_reduce(send))
    own_ends, other_ends = [], []
    for slots in GROUPS.values():
        a, b = finish([sums[slot] for slot in slots])
        own_ends.append(a)
        other_ends.append(from_core(b))
    groups = [sum((SLOTS[slot] for slot in slots), []) for slots in GROUPS.values()]
    out = place(out_mask, None, own_ends[:-1], other_ends[:-1], groups[:-1])
    return place(out_mask, out, own_ends[-1:], other_ends[-1:], groups[-1:])


def solution(mesh):
    in_specs = (P("row", "kk"), P("kk", "row"), P("row", "kk"), P("kk", "row"), P("row", None))
    out_specs = P(("row", "kk"), None)

    return jax.shard_map(per_device, mesh=mesh, in_specs=in_specs, out_specs=out_specs, check_vma=False)
```

```python
import functools

import jax
import jax.numpy as jnp
from jax import lax
from jax.experimental import pallas as pl
from jax.experimental.pallas import tpu as pltpu
from jax.sharding import PartitionSpec as P


Z, Y, C, X = 8, 4, 2, 4
BS = 128
BOTH = ("row", "kk")


def flat(z, y, c, x):
    return ((z * Y + y) * C + c) * X + x


def move(v, source):
    pairs = []
    for z in range(Z):
        for y in range(Y):
            for c in range(C):
                for x in range(X):
                    sz, sy, sc, sx = source(z, y, c, x)
                    pairs.append((flat(sz % Z, sy % Y, sc, sx), flat(z, y, c, x)))
    return lax.ppermute(v, BOTH, pairs)


def from_y(v, d):
    return move(v, lambda z, y, c, x: (z, y + d, c, x))


def from_z(v, d):
    return move(v, lambda z, y, c, x: (z + d, y, c, x))


def from_share(v):
    return move(v, lambda z, y, c, x: (z, y, c, x ^ 1))


def from_reduce(v):
    return move(v, lambda z, y, c, x: (z, y, c, X - 1 - x))


def from_core(v):
    return move(v, lambda z, y, c, x: (z, y, 1 - c, x))


def spread(v):
    return [from_y(v, d) for d in range(1, Y)]


def mask_right(right, mask):
    depth, cols = right.shape
    blocks = mask.shape[1]

    def body(mask_ref, right_ref, out_ref):
        for k in range(blocks):
            rows = pl.ds(k * BS, BS)
            out_ref[rows, :] = right_ref[rows, :] * mask_ref[0, k].astype(jnp.float32).astype(jnp.bfloat16)

    return pl.pallas_call(
        body,
        out_shape=jax.ShapeDtypeStruct((depth, cols), jnp.bfloat16),
        in_specs=[pl.BlockSpec(memory_space=pltpu.SMEM), pl.BlockSpec(memory_space=pltpu.VMEM)],
        out_specs=pl.BlockSpec(memory_space=pltpu.VMEM),
        compiler_params=pltpu.CompilerParams(vmem_limit_bytes=8 << 20),
        name="mask_right",
    )(mask, right)


def mask_left(left, mask, order):
    depth = left.shape[1]

    def body(order_ref, mask_ref, a_ref, b_ref, mine_ref, theirs_ref):
        i = pl.program_id(0)
        for src, dst, at in ((a_ref, mine_ref, order_ref[i]), (b_ref, theirs_ref, order_ref[i + 2])):
            for k in range(depth // BS):
                cols = pl.ds(k * BS, BS)
                dst[:, cols] = src[:, cols] * mask_ref[at, k].astype(jnp.float32).astype(jnp.bfloat16)

    out = jax.ShapeDtypeStruct((2 * BS, depth), jnp.bfloat16)
    return pl.pallas_call(
        body,
        out_shape=(out, out),
        grid_spec=pltpu.PrefetchScalarGridSpec(
            num_scalar_prefetch=2,
            grid=(2,),
            in_specs=[
                pl.BlockSpec((BS, depth), lambda i, o, m: (o[i], 0)),
                pl.BlockSpec((BS, depth), lambda i, o, m: (o[i + 2], 0)),
            ],
            out_specs=[pl.BlockSpec((BS, depth), lambda i, o, m: (i, 0))] * 2,
        ),
        compiler_params=pltpu.CompilerParams(vmem_limit_bytes=8 << 20),
        name="mask_left",
    )(order, mask, left, left)


TAIL = 16


def code(v):
    return jnp.clip(jnp.floor(v + 0.5), -32767.0, 32767.0).astype(jnp.int32).astype(jnp.int16)


def value(q):
    return q.astype(jnp.int32).astype(jnp.float32)


def partial_product(lhs, steps):
    rows, depth2 = lhs.shape
    depth, quarter, width, count = depth2 // 2, rows // 4, 2 * BS, len(steps)
    arrays = []
    for step in steps:
        for a, _ in step:
            if not any(a is b for b in arrays):
                arrays.append(a)

    def which(a):
        return next(i for i, b in enumerate(arrays) if a is b)

    def body(lhs_ref, *refs):
        ins, (send_ref, keep_ref, right_ref) = refs[: len(arrays)], refs[len(arrays) :]

        def fill(step):
            for j, (a, k) in enumerate(step):
                ref = ins[which(a)]
                block = ref[...] if k is None else ref[k]
                right_ref[pl.ds((j // 2) * depth, depth), pl.ds((j % 2) * BS, BS)] = block

        def multiply(i, _):
            for k, step in enumerate(steps):
                pl.when(i == k)(functools.partial(fill, step))
            out = jnp.dot(lhs_ref[...], right_ref[...], preferred_element_type=jnp.float32)
            cols = pl.ds(pl.multiple_of(i * width, width), width)
            keep_ref[:quarter, cols] = out[quarter : 2 * quarter]
            keep_ref[quarter:, cols] = out[3 * quarter :]
            upper, lower = out[:quarter], out[2 * quarter : 3 * quarter]
            most = jnp.max(jnp.maximum(jnp.abs(upper), jnp.abs(lower)), axis=0, keepdims=True)
            exponent = jnp.ceil(jnp.log2(jnp.maximum(most, 1e-30)))
            scale = jnp.exp2(15.0 - exponent)
            send_ref[:quarter, cols] = code(upper * scale)
            send_ref[quarter : 2 * quarter, cols] = code(lower * scale)
            send_ref[2 * quarter :, cols] = code(jnp.broadcast_to(exponent, (TAIL, width)))
            return 0

        lax.fori_loop(0, count, multiply, 0)

    sent = jax.ShapeDtypeStruct((2 * quarter + TAIL, count * width), jnp.int16)
    kept = jax.ShapeDtypeStruct((2 * quarter, count * width), jnp.float32)
    vmem = pl.BlockSpec(memory_space=pltpu.VMEM)
    return pl.pallas_call(
        body,
        out_shape=(sent, kept),
        in_specs=[vmem] * (1 + len(arrays)),
        out_specs=(vmem, vmem),
        scratch_shapes=[pltpu.VMEM((depth2, width), jnp.bfloat16)],
        compiler_params=pltpu.CompilerParams(vmem_limit_bytes=24 << 20),
        cost_estimate=pl.CostEstimate(
            flops=2 * rows * depth2 * count * width, bytes_accessed=(3 * count) << 19, transcendentals=0
        ),
        name="partial_product",
    )(lhs, *arrays)


def finish(parts):
    rows = parts[0][0].shape[0]
    half, count = rows // 2, len(parts)
    widths = [k.shape[1] for k, _ in parts]
    starts = [sum(widths[:i]) for i in range(count)]
    total = sum(widths)
    tall = 32

    def body(*refs):
        ins, ends = refs[: 2 * count], refs[2 * count :]
        for i in range(count):
            kept_ref, got_ref = ins[2 * i : 2 * i + 2]
            cols = pl.ds(starts[i], widths[i])
            unit = jnp.exp2(value(got_ref[rows:, :])[:1] - 15.0)
            for base, dst in zip((0, half), ends):

                def add(r, _, base=base, dst=dst, cols=cols, unit=unit, kept_ref=kept_ref, got_ref=got_ref):
                    src = pl.ds(pl.multiple_of(base + r * tall, tall), tall)
                    to = pl.ds(pl.multiple_of(r * tall, tall), tall)
                    dst[to, cols] = (kept_ref[src, :] + value(got_ref[src, :]) * unit).astype(jnp.bfloat16)
                    return 0

                lax.fori_loop(0, half // tall, add, 0)

    out = jax.ShapeDtypeStruct((half, total), jnp.bfloat16)
    vmem = pl.BlockSpec(memory_space=pltpu.VMEM)
    return pl.pallas_call(
        body,
        out_shape=(out, out),
        in_specs=[vmem] * (2 * count),
        out_specs=(vmem, vmem),
        compiler_params=pltpu.CompilerParams(vmem_limit_bytes=12 << 20),
        cost_estimate=pl.CostEstimate(flops=rows * total * 2, bytes_accessed=rows * total * 10, transcendentals=0),
        name="finish",
    )(*(v for pair in parts for v in pair))


def place(out_mask, base, own, other, groups):
    rows = own[0].shape[0]
    count = len(groups)
    blocks = 4 * sum(len(steps) for steps in groups)

    def body(mask_ref, *refs):
        ends, (out_ref, buf, sem) = refs[-3 - 2 * count : -3], refs[-3:]
        z, y, c, x = position()
        copies = []
        for g, steps in enumerate(groups):
            for p, (d, h) in enumerate(steps):
                for k in range(2):
                    group = lax.rem(z + d % Z, Z) * Y + lax.rem(y + 2 * h + k, Y)
                    for src, core in ((ends[g], c), (ends[count + g], 1 - c)):
                        i, block = len(copies), group * C + core
                        scale = mask_ref[x, block].astype(jnp.float32).astype(jnp.bfloat16)
                        buf[i] = src[:, pl.ds((2 * p + k) * BS, BS)] * scale
                        cols = pl.ds(pl.multiple_of(block * BS, BS), BS)
                        copies.append(pltpu.make_async_copy(buf.at[i], out_ref.at[:, cols], sem.at[i]))
                        copies[-1].start()
        for copy in copies:
            copy.wait()

    smem, vmem, hbm = (pl.BlockSpec(memory_space=m) for m in (pltpu.SMEM, pltpu.VMEM, pltpu.HBM))
    bases = [] if base is None else [base]
    return pl.pallas_call(
        body,
        out_shape=jax.ShapeDtypeStruct((rows, Z * Y * C * BS), jnp.bfloat16),
        in_specs=[smem] + [hbm] * len(bases) + [vmem] * (2 * count),
        out_specs=hbm,
        input_output_aliases={1: 0} if bases else {},
        scratch_shapes=[pltpu.VMEM((blocks, rows, BS), jnp.bfloat16), pltpu.SemaphoreType.DMA((blocks,))],
        compiler_params=pltpu.CompilerParams(vmem_limit_bytes=12 << 20),
        cost_estimate=pl.CostEstimate(flops=blocks * rows * BS, bytes_accessed=blocks * rows * BS * 4, transcendentals=0),
        name="place",
    )(out_mask, *bases, *own, *other)


def position():
    row, x = lax.axis_index("row"), lax.axis_index("kk")
    return row // (Y * C), (row // C) % Y, row % C, x


PAIRS = range(Y // 2)
SLOTS = {
    "0": [(0, h) for h in PAIRS],
    "4": [(4, h) for h in PAIRS],
    "1": [(d, h) for d in (1, -1) for h in PAIRS],
    "2": [(d, h) for d in (2, -2) for h in PAIRS],
    "3": [(d, h) for d in (3, -3) for h in PAIRS],
}
GROUPS = {"fin0": ("0", "1"), "fin1": ("2", "4"), "fin2": ("3",)}


def per_device(left_blocks, right_blocks, left_mask, right_mask, out_mask):
    x = lax.axis_index("kk")
    near = x + 1 - 2 * (x % 2)
    order = jnp.stack([X - 1 - x, x, X - 1 - near, near]).astype(jnp.int32)

    mine = mask_right(right_blocks, right_mask.T)
    theirs = from_share(mine)
    along = spread(mine)
    far = from_z(mine, 4)
    near_along = from_share(jnp.stack(along))
    own = {}
    line = {(0, 0): (theirs, None)}
    for k in range(1, Y):
        line[0, k] = (near_along, k - 1)

    hop = {}
    for s in (1, -1):
        first = from_z(theirs, s)
        line[s, 0] = (first, None)
        hop[s, 0] = jnp.stack([mine, *along, first])
        for d in (1, 2):
            packet = from_z(hop[s, d - 1], s)
            hop[s, d] = packet
            for k in range(Y):
                own[s * d, k] = (packet, k)
            line[s * (d + 1), 0] = (packet, Y)
        last = hop[s, 2][:Y]
        packet = from_z(last, s)
        for k in range(Y):
            own[s * 3, k] = (packet, k)
    for k in range(Y):
        own[0, k] = (hop[1, 0], k)

    def block(pair):
        array, index = pair
        return array if index is None else array[index]

    for d in (1, 2, 3):
        both = jnp.stack([block(line[d, 0]), block(line[-d, 0])])
        for k, got in enumerate(spread(both), 1):
            line[d, k], line[-d, k] = (got, 0), (got, 1)

    far_all = [far] + spread(far)
    near_far = from_share(jnp.stack(far_all))
    for k in range(Y):
        own[4, k], line[4, k] = (far_all[k], None), (near_far, k)

    own_rows, their_rows = mask_left(left_blocks, left_mask, order)
    half = jnp.concatenate([own_rows, from_share(their_rows)], axis=1)
    lhs = jnp.concatenate([half, from_core(half)], axis=0)

    sums = {}
    for slot, steps in SLOTS.items():
        send, keep = partial_product(
            lhs, [[table[d, 2 * h + k] for table in (own, line) for k in range(2)] for d, h in steps]
        )
        sums[slot] = (keep, from_reduce(send))
    own_ends, other_ends = [], []
    for slots in GROUPS.values():
        a, b = finish([sums[slot] for slot in slots])
        own_ends.append(a)
        other_ends.append(from_core(b))
    groups = [sum((SLOTS[slot] for slot in slots), []) for slots in GROUPS.values()]
    out = place(out_mask, None, own_ends[:-1], other_ends[:-1], groups[:-1])
    return place(out_mask, out, own_ends[-1:], other_ends[-1:], groups[-1:])


def solution(mesh):
    in_specs = (P("row", "kk"), P("kk", "row"), P("row", "kk"), P("kk", "row"), P("row", None))
    out_specs = P(("row", "kk"), None)

    return jax.shard_map(per_device, mesh=mesh, in_specs=in_specs, out_specs=out_specs, check_vma=False)
```

```python
import functools

import jax
import jax.numpy as jnp
from jax import lax
from jax.experimental import pallas as pl
from jax.experimental.pallas import tpu as pltpu
from jax.sharding import PartitionSpec as P


Z, Y, C, X = 8, 4, 2, 4
BS = 128
BOTH = ("row", "kk")


def flat(z, y, c, x):
    return ((z * Y + y) * C + c) * X + x


def move(v, source):
    pairs = []
    for z in range(Z):
        for y in range(Y):
            for c in range(C):
                for x in range(X):
                    sz, sy, sc, sx = source(z, y, c, x)
                    pairs.append((flat(sz % Z, sy % Y, sc, sx), flat(z, y, c, x)))
    return lax.ppermute(v, BOTH, pairs)


def from_y(v, d):
    return move(v, lambda z, y, c, x: (z, y + d, c, x))


def from_z(v, d):
    return move(v, lambda z, y, c, x: (z + d, y, c, x))


def from_share(v):
    return move(v, lambda z, y, c, x: (z, y, c, x ^ 1))


def from_reduce(v):
    return move(v, lambda z, y, c, x: (z, y, c, X - 1 - x))


def from_core(v):
    return move(v, lambda z, y, c, x: (z, y, 1 - c, x))


def spread(v):
    return [from_y(v, d) for d in range(1, Y)]


def mask_right(right, mask):
    depth, cols = right.shape
    blocks = mask.shape[1]

    def body(mask_ref, right_ref, out_ref):
        for k in range(blocks):
            rows = pl.ds(k * BS, BS)
            out_ref[rows, :] = right_ref[rows, :] * mask_ref[0, k].astype(jnp.float32).astype(jnp.bfloat16)

    return pl.pallas_call(
        body,
        out_shape=jax.ShapeDtypeStruct((depth, cols), jnp.bfloat16),
        in_specs=[pl.BlockSpec(memory_space=pltpu.SMEM), pl.BlockSpec(memory_space=pltpu.VMEM)],
        out_specs=pl.BlockSpec(memory_space=pltpu.VMEM),
        compiler_params=pltpu.CompilerParams(vmem_limit_bytes=8 << 20),
        name="mask_right",
    )(mask, right)


def mask_left(left, mask, order):
    depth = left.shape[1]

    def body(order_ref, mask_ref, a_ref, b_ref, mine_ref, theirs_ref):
        i = pl.program_id(0)
        for src, dst, at in ((a_ref, mine_ref, order_ref[i]), (b_ref, theirs_ref, order_ref[i + 2])):
            for k in range(depth // BS):
                cols = pl.ds(k * BS, BS)
                dst[:, cols] = src[:, cols] * mask_ref[at, k].astype(jnp.float32).astype(jnp.bfloat16)

    out = jax.ShapeDtypeStruct((2 * BS, depth), jnp.bfloat16)
    return pl.pallas_call(
        body,
        out_shape=(out, out),
        grid_spec=pltpu.PrefetchScalarGridSpec(
            num_scalar_prefetch=2,
            grid=(2,),
            in_specs=[
                pl.BlockSpec((BS, depth), lambda i, o, m: (o[i], 0)),
                pl.BlockSpec((BS, depth), lambda i, o, m: (o[i + 2], 0)),
            ],
            out_specs=[pl.BlockSpec((BS, depth), lambda i, o, m: (i, 0))] * 2,
        ),
        compiler_params=pltpu.CompilerParams(vmem_limit_bytes=8 << 20),
        name="mask_left",
    )(order, mask, left, left)


TAIL = 16


def code(v):
    return jnp.clip(jnp.floor(v + 0.5), -32767.0, 32767.0).astype(jnp.int32).astype(jnp.int16)


def value(q):
    return q.astype(jnp.int32).astype(jnp.float32)


def partial_product(lhs, steps):
    rows, depth2 = lhs.shape
    depth, quarter, width, count = depth2 // 2, rows // 4, 2 * BS, len(steps)
    arrays = []
    for step in steps:
        for a, _ in step:
            if not any(a is b for b in arrays):
                arrays.append(a)

    def which(a):
        return next(i for i, b in enumerate(arrays) if a is b)

    def body(lhs_ref, *refs):
        ins, (send_ref, keep_ref, right_ref) = refs[: len(arrays)], refs[len(arrays) :]

        def fill(step):
            for j, (a, k) in enumerate(step):
                ref = ins[which(a)]
                block = ref[...] if k is None else ref[k]
                right_ref[pl.ds((j // 2) * depth, depth), pl.ds((j % 2) * BS, BS)] = block

        def multiply(i, _):
            for k, step in enumerate(steps):
                pl.when(i == k)(functools.partial(fill, step))
            out = jnp.dot(lhs_ref[...], right_ref[...], preferred_element_type=jnp.float32)
            cols = pl.ds(pl.multiple_of(i * width, width), width)
            keep_ref[:quarter, cols] = out[quarter : 2 * quarter]
            keep_ref[quarter:, cols] = out[3 * quarter :]
            upper, lower = out[:quarter], out[2 * quarter : 3 * quarter]
            most = jnp.max(jnp.maximum(jnp.abs(upper), jnp.abs(lower)), axis=0, keepdims=True)
            exponent = jnp.ceil(jnp.log2(jnp.maximum(most, 1e-30)))
            scale = jnp.exp2(15.0 - exponent)
            send_ref[:quarter, cols] = code(upper * scale)
            send_ref[quarter : 2 * quarter, cols] = code(lower * scale)
            send_ref[2 * quarter :, cols] = code(jnp.broadcast_to(exponent, (TAIL, width)))
            return 0

        lax.fori_loop(0, count, multiply, 0)

    sent = jax.ShapeDtypeStruct((2 * quarter + TAIL, count * width), jnp.int16)
    kept = jax.ShapeDtypeStruct((2 * quarter, count * width), jnp.float32)
    vmem = pl.BlockSpec(memory_space=pltpu.VMEM)
    return pl.pallas_call(
        body,
        out_shape=(sent, kept),
        in_specs=[vmem] * (1 + len(arrays)),
        out_specs=(vmem, vmem),
        scratch_shapes=[pltpu.VMEM((depth2, width), jnp.bfloat16)],
        compiler_params=pltpu.CompilerParams(vmem_limit_bytes=24 << 20),
        cost_estimate=pl.CostEstimate(
            flops=2 * rows * depth2 * count * width, bytes_accessed=(3 * count) << 19, transcendentals=0
        ),
        name="partial_product",
    )(lhs, *arrays)


def finish(parts):
    rows = parts[0][0].shape[0]
    half, count = rows // 2, len(parts)
    widths = [k.shape[1] for k, _ in parts]
    starts = [sum(widths[:i]) for i in range(count)]
    total = sum(widths)
    tall = 32

    def body(*refs):
        ins, ends = refs[: 2 * count], refs[2 * count :]
        for i in range(count):
            kept_ref, got_ref = ins[2 * i : 2 * i + 2]
            cols = pl.ds(starts[i], widths[i])
            unit = jnp.exp2(value(got_ref[rows:, :])[:1] - 15.0)
            for base, dst in zip((0, half), ends):

                def add(r, _, base=base, dst=dst, cols=cols, unit=unit, kept_ref=kept_ref, got_ref=got_ref):
                    src = pl.ds(pl.multiple_of(base + r * tall, tall), tall)
                    to = pl.ds(pl.multiple_of(r * tall, tall), tall)
                    dst[to, cols] = (kept_ref[src, :] + value(got_ref[src, :]) * unit).astype(jnp.bfloat16)
                    return 0

                lax.fori_loop(0, half // tall, add, 0)

    out = jax.ShapeDtypeStruct((half, total), jnp.bfloat16)
    vmem = pl.BlockSpec(memory_space=pltpu.VMEM)
    return pl.pallas_call(
        body,
        out_shape=(out, out),
        in_specs=[vmem] * (2 * count),
        out_specs=(vmem, vmem),
        compiler_params=pltpu.CompilerParams(vmem_limit_bytes=12 << 20),
        cost_estimate=pl.CostEstimate(flops=rows * total * 2, bytes_accessed=rows * total * 10, transcendentals=0),
        name="finish",
    )(*(v for pair in parts for v in pair))


def place(out_mask, base, own, other, groups):
    rows = own[0].shape[0]
    count = len(groups)
    blocks = 4 * sum(len(steps) for steps in groups)

    def body(mask_ref, *refs):
        ends, (out_ref, buf, sem) = refs[-3 - 2 * count : -3], refs[-3:]
        z, y, c, x = position()
        copies = []
        for g, steps in enumerate(groups):
            for p, (d, h) in enumerate(steps):
                for k in range(2):
                    group = lax.rem(z + d % Z, Z) * Y + lax.rem(y + 2 * h + k, Y)
                    for src, core in ((ends[g], c), (ends[count + g], 1 - c)):
                        i, block = len(copies), group * C + core
                        scale = mask_ref[x, block].astype(jnp.float32).astype(jnp.bfloat16)
                        buf[i] = src[:, pl.ds((2 * p + k) * BS, BS)] * scale
                        cols = pl.ds(pl.multiple_of(block * BS, BS), BS)
                        copies.append(pltpu.make_async_copy(buf.at[i], out_ref.at[:, cols], sem.at[i]))
                        copies[-1].start()
        for copy in copies:
            copy.wait()

    smem, vmem, hbm = (pl.BlockSpec(memory_space=m) for m in (pltpu.SMEM, pltpu.VMEM, pltpu.HBM))
    bases = [] if base is None else [base]
    return pl.pallas_call(
        body,
        out_shape=jax.ShapeDtypeStruct((rows, Z * Y * C * BS), jnp.bfloat16),
        in_specs=[smem] + [hbm] * len(bases) + [vmem] * (2 * count),
        out_specs=hbm,
        input_output_aliases={1: 0} if bases else {},
        scratch_shapes=[pltpu.VMEM((blocks, rows, BS), jnp.bfloat16), pltpu.SemaphoreType.DMA((blocks,))],
        compiler_params=pltpu.CompilerParams(vmem_limit_bytes=12 << 20),
        cost_estimate=pl.CostEstimate(flops=blocks * rows * BS, bytes_accessed=blocks * rows * BS * 4, transcendentals=0),
        name="place",
    )(out_mask, *bases, *own, *other)


def position():
    row, x = lax.axis_index("row"), lax.axis_index("kk")
    return row // (Y * C), (row // C) % Y, row % C, x


PAIRS = range(Y // 2)
SLOTS = {
    "0": [(0, h) for h in PAIRS],
    "4": [(4, h) for h in PAIRS],
    "1": [(d, h) for d in (1, -1) for h in PAIRS],
    "2": [(d, h) for d in (2, -2) for h in PAIRS],
    "3": [(d, h) for d in (3, -3) for h in PAIRS],
}
GROUPS = {"fin0": ("0", "1"), "fin1": ("2", "4"), "fin2": ("3",)}


def per_device(left_blocks, right_blocks, left_mask, right_mask, out_mask):
    x = lax.axis_index("kk")
    near = x + 1 - 2 * (x % 2)
    order = jnp.stack([X - 1 - x, x, X - 1 - near, near]).astype(jnp.int32)

    mine = mask_right(right_blocks, right_mask.T)
    theirs = from_share(mine)
    along = spread(mine)
    near_along = from_share(jnp.stack(along))
    own = {}
    line = {(0, 0): (theirs, None)}
    for k in range(1, Y):
        line[0, k] = (near_along, k - 1)

    hop = {0: jnp.stack([mine, *along])}
    single = {0: theirs}
    for d in (1, 2, 3):
        for s in (1, -1):
            single[s * d] = from_z(single[s * (d - 1)], s)
            hop[s * d] = from_z(hop[s * (d - 1)], s)
    for d, packet in hop.items():
        for k in range(Y):
            own[d, k] = (packet, k)

    for d in (1, 2, 3):
        line[d, 0], line[-d, 0] = (single[d], None), (single[-d], None)
        both = jnp.stack([single[d], single[-d]])
        for k, got in enumerate(spread(both), 1):
            line[d, k], line[-d, k] = (got, 0), (got, 1)

    far = from_z(single[3], 1)
    far_all = [far] + spread(far)
    near_far = from_share(jnp.stack(far_all))
    for k in range(Y):
        line[4, k], own[4, k] = (far_all[k], None), (near_far, k)

    own_rows, their_rows = mask_left(left_blocks, left_mask, order)
    half = jnp.concatenate([own_rows, from_share(their_rows)], axis=1)
    lhs = jnp.concatenate([half, from_core(half)], axis=0)

    sums = {}
    for slot, steps in SLOTS.items():
        send, keep = partial_product(
            lhs, [[table[d, 2 * h + k] for table in (own, line) for k in range(2)] for d, h in steps]
        )
        sums[slot] = (keep, from_reduce(send))
    own_ends, other_ends = [], []
    for slots in GROUPS.values():
        a, b = finish([sums[slot] for slot in slots])
        own_ends.append(a)
        other_ends.append(from_core(b))
    groups = [sum((SLOTS[slot] for slot in slots), []) for slots in GROUPS.values()]
    out = place(out_mask, None, own_ends[:-1], other_ends[:-1], groups[:-1])
    return place(out_mask, out, own_ends[-1:], other_ends[-1:], groups[-1:])


def solution(mesh):
    in_specs = (P("row", "kk"), P("kk", "row"), P("row", "kk"), P("kk", "row"), P("row", None))
    out_specs = P(("row", "kk"), None)

    return jax.shard_map(per_device, mesh=mesh, in_specs=in_specs, out_specs=out_specs, check_vma=False)
```
